256 devices in a mesh: groups: 4 (over x, y), seq: 64 (over z, core).
Axes of the slice: x: 2, y: 2, z: 32, core: 2. Of those that a mesh axis runs over, the one named last changes fastest.
The devices are a block of a 4x8x32 slice.
Arguments:
- queries: bfloat16 [32768, 4096], P(('groups', 'seq')), parts along dimension 0, may hold values from -100 to 100
- keys_values: bfloat16 [32768, 2, 512], P(('groups', 'seq')), parts along dimension 0, may hold values from -5 to 5
- head_signs: int32 [32, 128], replicated, may hold values from -1 to 1, as said below
- out_codes: int32 [512, 8192], P(None, 'seq'), may hold values from -2147483648 to 2147483647, as said below
- out_scales: bfloat16 [32, 8192], replicated, may hold values from 0.019897461 to 0.19921875
Outputs:
- projected: bfloat16 [32768, 8192], P(('groups', 'seq')), parts along dimension 0
The draws below stay inside these ranges and needn't reach their ends.
There are 4 independent parts, one for each index of `groups`. The reference program is written for one: setup_inputs(seed, part) draws one part's arguments, and reference() takes and returns one part's arrays. A program takes and returns all parts, laid end to end along the dimension named above; an argument that names none is the same for every part. Nothing has to cross between parts.
Inputs may be any that keep to these rules, and one draw needn't show every extreme that they name: `head_signs`: every entry is -1 or 1. `out_codes`: each word holds eight codes of 0 to 15, the code of row 8 i + k in bits 4k to 4k + 3 of word row i, the word read as a signed 32-bit integer.
All inputs are finite; a program needn't handle non-finite values.
Results may differ from the reference program's by a relative error of at most 0.006.
Values may be sent and summed in bfloat16 or wider, within the bound.
A program may use at most 128 MiB of HBM per device.

```python
import functools
import math
import jax
import jax.numpy as jnp
from jax import lax

D = 8192
HEADS = 32
KV = 4
HD = 128
GROUP = 128
WINDOW = 2048
TOKENS = 8192


def pair_draw(key):
    query_key = jax.random.fold_in(key, 101)
    kv_key = jax.random.fold_in(key, 102)
    base_queries = jnp.clip(jax.random.normal(query_key, (TOKENS, HEADS * HD), jnp.float32), -4.5, 4.5)
    base_kv = jnp.clip(jax.random.normal(kv_key, (TOKENS, 2, KV * HD), jnp.float32), -4.5, 4.5)
    return (base_queries, base_kv)


def draw_queries(key, part):
    return pair_draw(key)[0].astype(jnp.bfloat16)


def draw_keys_values(key, part):
    return pair_draw(key)[1].astype(jnp.bfloat16)


def draw_head_signs(key, part):
    sign_key = jax.random.fold_in(key, 301)
    return (2 * jax.random.randint(sign_key, (HEADS, HD), 0, 2, jnp.int32) - 1).astype(jnp.int32)


def draw_out_codes(key, part):
    code_key = jax.random.fold_in(key, 401)
    nibbles = jax.random.randint(code_key, (HEADS * HD // 8, D, 8), 0, 16, jnp.int32)
    shifted = [jnp.left_shift(nibbles[:, :, nibble_index], 4 * nibble_index) for nibble_index in range(8)]
    return functools.reduce(jnp.bitwise_or, shifted).astype(jnp.int32)


def setup_inputs(seed: int = 0, part: int = 0) -> dict:
    splits = jax.random.split(jax.random.key(seed), 6)
    part_keys = jax.random.split(jax.random.fold_in(splits[5], part), 6)
    return {
        "queries": draw_queries(jax.random.fold_in(jax.random.fold_in(splits[5], part), 71), part),
        "keys_values": draw_keys_values(jax.random.fold_in(jax.random.fold_in(splits[5], part), 71), part),
        "head_signs": draw_head_signs(jax.random.fold_in(splits[5], 71), part),
        "out_codes": draw_out_codes(jax.random.fold_in(splits[5], 71), part),
        "out_scales": jnp.clip(jnp.exp(jax.random.uniform(splits[4], (HEADS * HD // GROUP, D), jnp.float32, math.log(0.019897461), math.log(0.19921875))), 0.019897461, 0.19921875).astype(jnp.bfloat16),
    }


def hadamard(order):
    index = jnp.arange(order, dtype=jnp.int32)
    common = jnp.bitwise_and(index[:, None], index[None, :])
    ones = jnp.zeros((order, order), jnp.int32)
    for bit_index in range(order.bit_length()):
        ones = ones + jnp.bitwise_and(jnp.right_shift(common, bit_index), 1)
    return jnp.where(ones % 2 == 0, 1.0, -1.0).astype(jnp.float32)

def unpack(code_words):
    nibbles = [jnp.bitwise_and(jnp.right_shift(code_words, 4 * nibble_index), 15) for nibble_index in range(8)]
    stacked = jnp.stack(nibbles, axis=1)
    stacked = stacked.reshape(code_words.shape[0] * 8, code_words.shape[1])
    return (stacked - 8).astype(jnp.float32)

def rotate(attended, head_signs):
    signed = attended * head_signs.astype(jnp.float32)[None]
    mixed = jnp.einsum('thd,de->the', signed, hadamard(HD), precision=lax.Precision.HIGHEST) / math.sqrt(HD)
    return mixed.astype(jnp.bfloat16).reshape(attended.shape[0], HEADS * HD)

def reference(queries, keys_values, head_signs, out_codes, out_scales):
    per_group = HEADS // KV
    block_rows = math.gcd(TOKENS, 512)
    block_count = TOKENS // block_rows
    key_count = WINDOW + block_rows
    padded = jnp.concatenate([jnp.zeros((WINDOW, 2, KV * HD), keys_values.dtype), keys_values], axis=0)

    def attend(block):
        start = (block * block_rows).astype(jnp.int32)
        query_rows = lax.dynamic_slice_in_dim(queries, start, block_rows, 0).astype(jnp.float32)
        query_rows = query_rows.reshape(block_rows, KV, per_group, HD)
        key_value = lax.dynamic_slice_in_dim(padded, start, key_count, 0).astype(jnp.float32)
        key_rows = key_value[:, 0].reshape(key_count, KV, HD)
        value_rows = key_value[:, 1].reshape(key_count, KV, HD)
        scores = jnp.einsum('iGhd,jGd->Ghij', query_rows, key_rows) / math.sqrt(HD)
        query_pos = start + jnp.arange(block_rows, dtype=jnp.int32)
        key_pos = start - WINDOW + jnp.arange(key_count, dtype=jnp.int32)
        distance = query_pos[:, None] - key_pos[None, :]
        allowed = (distance >= 0) & (distance < WINDOW) & (key_pos[None, :] >= 0)
        allowed = allowed[None, None]
        scores = jnp.where(allowed, scores, -jnp.inf)
        row_max = lax.optimization_barrier(jnp.max(scores, axis=-1, keepdims=True))
        weights = jnp.where(allowed, jnp.exp(scores - row_max), 0.0)
        total = lax.optimization_barrier(jnp.sum(weights, axis=-1, keepdims=True))
        rounded = lax.optimization_barrier(weights.astype(jnp.bfloat16)).astype(jnp.float32)
        weighted = jnp.einsum('Ghij,jGd->Ghid', rounded, value_rows) / total
        return jnp.transpose(weighted, (2, 0, 1, 3)).reshape(block_rows, HEADS, HD)
    attended = lax.map(attend, jnp.arange(block_count, dtype=jnp.int32)).reshape(TOKENS, HEADS, HD)
    rotated = rotate(attended, head_signs)
    code_vals = unpack(out_codes)
    scaled = code_vals.reshape(HEADS * HD // GROUP, GROUP, D) * out_scales.astype(jnp.float32)[:, None, :]
    weight = scaled.reshape(HEADS * HD, D).astype(jnp.bfloat16)
    return jnp.dot(rotated, weight, preferred_element_type=jnp.float32).astype(jnp.bfloat16)
```

```python
import functools
import math

import jax
import jax.numpy as jnp
import numpy as np
from jax import lax
from jax.experimental import pallas as pl
from jax.experimental.pallas import tpu as pltpu
from jax.sharding import PartitionSpec as P

HEADS = 32
KV = 4
HD = 128
WINDOW = 2048
CORES = 2
MESH = pl.DeviceIdType.MESH
F32 = jnp.float32
BF16 = jnp.bfloat16


def hadamard_columns():
    d = np.arange(HD)
    e = np.array([8 * i + k for k in range(8) for i in range(HD // 8)])
    common = d[:, None] & e[None, :]
    bits = sum((common >> b) & 1 for b in range(HD.bit_length()))
    return np.where(bits % 2 == 0, 1.0, -1.0).astype(np.float32)


def kernel(
    plane_y,
    queries, kvt, codes_in, scales, signs, had,
    out,
    codes, kv, q, acc, top, xr, wbuf, obuf, sc,
    zm_recv, zp_recv, kv_recv, xy_recv,
    zm_send, zp_send, kv_send, xy_send,
    load_sem, pair_send, pair_recv, xr_send, xr_recv, out_local, out_send, out_recv,
):
    ns = lax.axis_size("seq")
    nz = ns // CORES
    g = lax.axis_index("groups")
    s = lax.axis_index("seq")
    z = s // CORES
    c = s % CORES
    tok = queries.shape[0]
    rows = tok * CORES
    half_heads = HEADS // CORES
    width = half_heads * HD
    hops = WINDOW // rows
    words = codes_in.shape[0]
    half, quarter = words // 2, words // 4

    gx_, gy_ = g // plane_y, g % plane_y
    across_x = (gx_ + 1 - 2 * (gx_ % 2)) * plane_y + gy_
    across_y = gx_ * plane_y + gy_ + 1 - 2 * (gy_ % 2)
    parity = (gx_ + gy_) % 2
    partner = (g, z * CORES + 1 - c)
    up = (g, (s + CORES) % ns)
    down = (g, (s + ns - CORES) % ns)

    down_steps_a = 3 * hops // 2
    up_steps = (nz - 1 - down_steps_a) // 2 + 1
    down_steps = nz - 1 - up_steps

    barrier = pltpu.get_barrier_semaphore()
    for dev in (partner, up, down, (across_x, s), (across_y, s)):
        pl.semaphore_signal(barrier, inc=1, device_id=dev, device_id_type=MESH)
    pl.semaphore_wait(barrier, 5)

    def remote(src, dst, send_sem, recv_sem, dev):
        return pltpu.make_async_remote_copy(
            src_ref=src, dst_ref=dst, send_sem=send_sem, recv_sem=recv_sem, device_id=dev, device_id_type=MESH
        )

    load_codes = pltpu.make_async_copy(codes_in, codes.at[z], load_sem.at[0])
    load_codes.start()
    load_kv = pltpu.make_async_copy(kvt.at[c], kv.at[0, :, pl.ds(c * tok, tok)], load_sem.at[1])
    load_kv.start()
    give_kv = remote(kvt.at[1 - c], kv.at[0, :, pl.ds(c * tok, tok)], pair_send.at[0], pair_recv.at[0], partner)
    give_kv.start()
    load_q = pltpu.make_async_copy(
        queries.at[:, pl.ds(pl.multiple_of(c * width, HD), width)], q.at[pl.ds(c * tok, tok)], load_sem.at[2]
    )
    load_q.start()
    give_q = remote(
        queries.at[:, pl.ds(pl.multiple_of((1 - c) * width, HD), width)],
        q.at[pl.ds(c * tok, tok)], pair_send.at[1], pair_recv.at[1], partner,
    )
    give_q.start()

    def part(block, a):
        return codes.at[block, pl.ds(pl.multiple_of(parity * half + a * quarter, quarter), quarter)]

    def share(block, a):
        dev = across_x + a * (across_y - across_x)
        ref = part(block, a)
        remote(ref, ref, xy_send.at[0], xy_recv.at[a * nz + block], (dev, s)).start()

    def zm_first(a):
        ref = part(z, a)
        remote(ref, ref, zm_send.at[0], zm_recv.at[a], down).start()

    def zp_first(a):
        ref = part(z, a)
        remote(ref, ref, zp_send.at[0], zp_recv.at[a], up).start()

    def zm_step(step, a):
        block = (z + step) % nz
        ref = part(block, a)
        remote(ref, ref, zm_send.at[0], zm_recv.at[(step - 1) * 2 + a], down).wait_recv()

        @pl.when(step < down_steps)
        def _():
            remote(ref, ref, zm_send.at[0], zm_recv.at[step * 2 + a], down).start()

        share(block, a)

    def zp_step(step, a):
        block = (z + nz - step) % nz
        ref = part(block, a)
        remote(ref, ref, zp_send.at[0], zp_recv.at[(step - 1) * 2 + a], up).wait_recv()

        @pl.when(step < up_steps)
        def _():
            remote(ref, ref, zp_send.at[0], zp_recv.at[step * 2 + a], up).start()

        share(block, a)

    def half_step(e):
        step, a = e // 2 + 1, e % 2

        @pl.when(step + down_steps_a <= down_steps)
        def _():
            zm_step(step + down_steps_a, a)

        @pl.when(step <= up_steps)
        def _():
            zp_step(step, a)

    load_codes.wait()
    zm_first(0)
    zm_first(1)
    load_kv.wait()
    mine = kv.at[0, :, pl.ds((1 - c) * tok, tok)]
    remote(mine, mine, pair_send.at[0], pair_recv.at[0], partner).wait_recv()

    def kv_send_from(t, part_index):
        ref = kv.at[t, part_index]
        remote(ref, kv.at[t + 1, part_index], kv_send.at[0], kv_recv.at[t * 4 + part_index], up).start()

    for part_index in range(4):
        kv_send_from(0, part_index)
    load_q.wait()
    mine = q.at[pl.ds((1 - c) * tok, tok)]
    remote(mine, mine, pair_send.at[1], pair_recv.at[1], partner).wait_recv()

    factor = math.log2(math.e) / math.sqrt(HD)

    def attend(t, head, group, mode):
        q_rows = q[:, pl.ds(pl.multiple_of(head * HD, HD), HD)]
        scores = lax.dot_general(
            q_rows, kv[t, 2 * group], (((1,), (1,)), ((), ())), preferred_element_type=F32
        )
        if mode != "full":
            i = lax.broadcasted_iota(jnp.int32, (rows, rows), 0)
            j = lax.broadcasted_iota(jnp.int32, (rows, rows), 1)
            scores = jnp.where(j <= i if mode == "own" else j > i, scores, -1e30)
        row_max = jnp.max(scores, axis=1, keepdims=True)
        if mode == "own":
            new_top = jnp.broadcast_to(row_max, (rows, HD))
        else:
            old_top = top[head]
            new_top = jnp.maximum(old_top, row_max)
        top[head] = new_top
        spread = jnp.concatenate([new_top] * (rows // HD), axis=1)
        weights = jnp.exp2((scores - spread) * factor).astype(BF16)
        values = jnp.concatenate([kv[t, 2 * group + 1], jnp.ones((rows, HD), BF16)], axis=1)
        product = jnp.dot(weights, values, preferred_element_type=F32)
        if mode != "own":
            fade = jnp.exp2((old_top - new_top) * factor)
            product = product + acc[head] * jnp.concatenate([fade, fade], axis=1)
        acc[head] = product

    quad = half_heads // 4

    def attend_quad(t, index, mode):
        def two(i, carry):
            head = index * quad + 2 * i
            attend(t, head, index // 2, mode)
            attend(t, head + 1, index // 2, mode)
            return carry

        lax.fori_loop(0, quad // 2, two, 0)

    def phase_a(t, carry):
        for index in range(4):
            ref = kv.at[t, index]
            remote(ref, ref, kv_send.at[0], kv_recv.at[(t - 1) * 4 + index], up).wait_recv()

            @pl.when(t < hops)
            def _():
                kv_send_from(t, index)

            if index < 3:
                e = (t - 1) * 3 + index
                zm_step(e // 2 + 1, e % 2)

            @pl.when(t == 1)
            def _():
                attend_quad(0, index, "own")

            @pl.when((t > 1) & (z >= t - 1))
            def _():
                attend_quad(t - 1, index, "full")

        return carry

    lax.fori_loop(1, hops + 1, phase_a, 0)
    zp_first(0)
    zp_first(1)
    for index in range(4):
        half_step(jnp.int32(index))

        @pl.when(z >= hops)
        def _():
            attend_quad(hops, index, "far")

    matrix = had[...]
    stacked = jnp.concatenate([matrix, matrix], axis=0)

    def rotate(head):
        both = acc[head]
        value = both[:, :HD] / both[:, HD:] * signs[c * half_heads + head]
        first = value.astype(BF16)
        rest = value - first.astype(F32)
        second = rest.astype(BF16)
        third = (rest - second.astype(F32)).astype(BF16)
        mixed = jnp.dot(jnp.concatenate([first, second], axis=1), stacked, preferred_element_type=F32)
        mixed = mixed + jnp.dot(third, matrix, preferred_element_type=F32)
        column = pl.multiple_of((c * half_heads + head) * HD, HD)
        xr[:, pl.ds(column, HD)] = (mixed * (1.0 / math.sqrt(HD))).astype(BF16)

    def rotate_two(i, carry):
        rotate(2 * i)
        rotate(2 * i + 1)
        return carry

    lax.fori_loop(0, half_heads // 4, rotate_two, 0)
    half_step(jnp.int32(4))
    lax.fori_loop(half_heads // 4, half_heads // 2, rotate_two, 0)
    half_step(jnp.int32(5))
    my_columns = xr.at[:, pl.ds(pl.multiple_of(c * width, HD), width)]
    swap = remote(my_columns, my_columns, xr_send.at[0], xr_recv.at[0], partner)
    swap.start()

    pairs = nz // 2
    first_pairs = down_steps_a // 2

    def origins(u):
        late = (u // first_pairs + 1) // 2
        k = u - first_pairs
        one = (1 - late) * 2 * u + late * (down_steps_a + k)
        two = (1 - late) * (2 * u + 1) + late * (nz - 1 - k)
        return (z + one) % nz, (z + two) % nz

    def unpack(block, side):
        column = pl.multiple_of((block * CORES + c) * HD, HD)
        sc[...] = scales[:, pl.ds(column, HD)].astype(F32)

        def eight_heads(i, carry):
            scale_rows = sc[pl.ds(pl.multiple_of(i * 8, 8), 8), :]
            for n in range(8):
                start = pl.multiple_of(i * HD + n * (HD // 8), HD // 8)
                packed = codes[block, pl.ds(start, HD // 8), :] ^ jnp.int32(-2004318072)
                scale = jnp.broadcast_to(scale_rows[n : n + 1, :], (HD // 8, HD))
                for k in range(8):
                    shifted = packed << (28 - 4 * k) if k < 7 else packed
                    value = (shifted >> 28).astype(F32)
                    at = pl.multiple_of((i * 8 + n) * HD + k * (HD // 8), HD // 8)
                    wbuf[pl.ds(at, HD // 8), side * HD : (side + 1) * HD] = (value * scale).astype(BF16)
            return carry

        lax.fori_loop(0, HEADS // 8, eight_heads, 0)

    def send_out(u):
        for side, block in enumerate(origins(u)):
            columns = pl.ds(pl.multiple_of((block * CORES + c) * HD, HD), HD)
            pltpu.make_async_copy(
                obuf.at[u, side, pl.ds(c * tok, tok)], out.at[:, columns], out_local.at[0]
            ).start()
            remote(
                obuf.at[u, side, pl.ds((1 - c) * tok, tok)], out.at[:, columns], out_send.at[0], out_recv.at[0], partner
            ).start()

    def shared(block):
        for a in range(2):
            ref = codes.at[block, pl.ds(pl.multiple_of((1 - parity) * half + a * quarter, quarter), quarter)]
            dev = across_x if a == 0 else across_y
            remote(ref, ref, xy_send.at[0], xy_recv.at[a * nz + block], (dev, s)).wait_recv()

    def project(u, carry):
        half_step(u + 6)

        @pl.when(u == 0)
        def _():
            theirs = xr.at[:, pl.ds(pl.multiple_of((1 - c) * width, HD), width)]
            remote(theirs, theirs, xr_send.at[0], xr_recv.at[0], partner).wait_recv()

        one, two = origins(u)

        @pl.when(u > 0)
        def _():
            shared(one)

        shared(two)
        unpack(one, 0)
        unpack(two, 1)
        total = jnp.dot(xr[...], wbuf[...], preferred_element_type=F32).astype(BF16)
        obuf[u, 0] = total[:, :HD]
        obuf[u, 1] = total[:, HD:]

        @pl.when(u > 0)
        def _():
            send_out(u - 1)

        return carry

    lax.fori_loop(0, pairs, project, 0)

    sent = codes.at[pl.ds(0, down_steps), pl.ds(0, half)]
    remote(sent, sent, zm_send.at[0], zm_recv.at[0], down).wait_send()
    sent = codes.at[pl.ds(0, up_steps), pl.ds(0, half)]
    remote(sent, sent, zp_send.at[0], zp_recv.at[0], up).wait_send()
    sent = codes.at[pl.ds(0, nz - 1), pl.ds(0, half)]
    remote(sent, sent, xy_send.at[0], xy_recv.at[0], (across_x, s)).wait_send()
    sent = kv.at[pl.ds(0, hops)]
    remote(sent, sent, kv_send.at[0], kv_recv.at[0], up).wait_send()
    give_kv.wait_send()
    give_q.wait_send()
    swap.wait_send()
    send_out(pairs - 1)
    moved = obuf.at[:, :, pl.ds(0, tok)]
    pltpu.make_async_copy(moved, moved, out_local.at[0]).wait()
    whole = remote(moved, moved, out_send.at[0], out_recv.at[0], partner)
    whole.wait_send()
    whole.wait_recv()


def on_device(plane_y, queries, keys_values, head_signs, out_codes, out_scales):
    tok = queries.shape[0]
    ns = lax.axis_size("seq")
    nz = ns // CORES
    rows = tok * CORES
    hops = WINDOW // rows
    words, cols = out_codes.shape
    half_heads = HEADS // CORES
    down_steps_a = 3 * hops // 2
    up_steps = (nz - 1 - down_steps_a) // 2 + 1
    down_steps = nz - 1 - up_steps
    kvt = keys_values.reshape(tok, 2, CORES, KV // CORES, HD)
    kvt = jnp.transpose(kvt, (2, 3, 1, 0, 4)).reshape(CORES, KV, tok, HD)
    signs = head_signs.astype(F32).reshape(HEADS, 1, HD)
    had = jnp.asarray(hadamard_columns(), BF16)
    hbm = pl.BlockSpec(memory_space=pltpu.HBM)
    vmem = pl.BlockSpec(memory_space=pltpu.VMEM)
    dma = pltpu.SemaphoreType.DMA
    return pl.pallas_call(
        functools.partial(kernel, plane_y),
        out_shape=jax.ShapeDtypeStruct((tok, ns * cols), BF16),
        in_specs=[hbm, hbm, hbm, vmem, vmem, vmem],
        out_specs=hbm,
        scratch_shapes=[
            pltpu.VMEM((nz, words, cols), jnp.int32),
            pltpu.VMEM((hops + 1, KV, rows, HD), BF16),
            pltpu.VMEM((rows, half_heads * HD), BF16),
            pltpu.VMEM((half_heads, rows, 2 * HD), F32),
            pltpu.VMEM((half_heads, rows, HD), F32),
            pltpu.VMEM((rows, HEADS * HD), BF16),
            pltpu.VMEM((HEADS * HD, 2 * cols), BF16),
            pltpu.VMEM((nz // 2, 2, rows, cols), BF16),
            pltpu.VMEM((HEADS, HD), F32),
            dma((2 * down_steps,)),
            dma((2 * up_steps,)),
            dma((4 * hops,)),
            dma((2 * nz,)),
            dma((1,)),
            dma((1,)),
            dma((1,)),
            dma((1,)),
            dma((3,)),
            dma((2,)),
            dma((2,)),
            dma((1,)),
            dma((1,)),
            dma((1,)),
            dma((1,)),
            dma((1,)),
        ],
        compiler_params=pltpu.CompilerParams(
            collective_id=0, has_side_effects=True, vmem_limit_bytes=60 * 1024 * 1024
        ),
    )(queries, kvt, out_codes, out_scales, signs, had)


def solution(mesh):
    groups = mesh.shape["groups"]
    plane_y = 1 << (groups.bit_length() // 2)
    return jax.shard_map(
        functools.partial(on_device, plane_y),
        mesh=mesh,
        in_specs=(
            P(("groups", "seq"), None),
            P(("groups", "seq"), None, None),
            P(),
            P(None, "seq"),
            P(),
        ),
        out_specs=P(("groups", "seq"), None),
        check_vma=False,
    )
```

```python
import functools
import math

import jax
import jax.numpy as jnp
import numpy as np
from jax import lax
from jax.experimental import pallas as pl
from jax.experimental.pallas import tpu as pltpu
from jax.sharding import PartitionSpec as P

HEADS = 32
KV = 4
HD = 128
WINDOW = 2048
CORES = 2
MESH = pl.DeviceIdType.MESH
F32 = jnp.float32
BF16 = jnp.bfloat16


def hadamard_columns():
    d = np.arange(HD)
    e = np.array([8 * i + k for k in range(8) for i in range(HD // 8)])
    common = d[:, None] & e[None, :]
    bits = sum((common >> b) & 1 for b in range(HD.bit_length()))
    return np.where(bits % 2 == 0, 1.0, -1.0).astype(np.float32)


def kernel(
    plane_y,
    queries, kv_in, codes_in, scales, signs, had,
    out,
    codes, kv, q, acc, top, xr, weights_even, weights_odd, partial, obuf,
    zm_recv, zp_recv, kv_recv, xy_recv,
    zm_send, zp_send, kv_send, xy_send,
    load_sem, pair_send, pair_recv, xr_send, xr_recv, out_local, out_send, out_recv,
):
    ns = lax.axis_size("seq")
    nz = ns // CORES
    g = lax.axis_index("groups")
    s = lax.axis_index("seq")
    z = s // CORES
    c = s % CORES
    tok = queries.shape[0]
    rows = tok * CORES
    half_heads = HEADS // CORES
    width = half_heads * HD
    hops = WINDOW // rows
    words = codes_in.shape[0]
    half, quarter, eighth = words // 2, words // 4, words // 8

    gx_, gy_ = g // plane_y, g % plane_y
    across_x = (gx_ + 1 - 2 * (gx_ % 2)) * plane_y + gy_
    across_y = gx_ * plane_y + gy_ + 1 - 2 * (gy_ % 2)
    parity = (gx_ + gy_) % 2
    partner = (g, z * CORES + 1 - c)
    up = (g, (s + CORES) % ns)
    down = (g, (s + ns - CORES) % ns)

    down_steps_a, up_steps, down_steps = plan(nz, hops)

    barrier = pltpu.get_barrier_semaphore()
    for dev in (partner, up, down, (across_x, s), (across_y, s)):
        pl.semaphore_signal(barrier, inc=1, device_id=dev, device_id_type=MESH)
    pl.semaphore_wait(barrier, 5)

    def remote(src, dst, send_sem, recv_sem, dev):
        return pltpu.make_async_remote_copy(
            src_ref=src, dst_ref=dst, send_sem=send_sem, recv_sem=recv_sem, device_id=dev, device_id_type=MESH
        )

    load_codes = pltpu.make_async_copy(codes_in, codes.at[z], load_sem.at[0])
    load_codes.start()
    loads, gives = [], []
    for part_index in range(KV):
        for core, into in ((c, loads), (1 - c, gives)):
            column = (part_index % 2) * KV * HD + (core * (KV // CORES) + part_index // 2) * HD
            source = kv_in.at[:, pl.ds(pl.multiple_of(column, HD), HD)]
            target = kv.at[0, part_index, pl.ds(c * tok, tok)]
            if into is loads:
                copy = pltpu.make_async_copy(source, target, load_sem.at[2 + part_index])
            else:
                copy = remote(source, target, pair_send.at[1 + part_index], pair_recv.at[1 + part_index], partner)
            copy.start()
            into.append(copy)
    load_q = pltpu.make_async_copy(
        queries.at[:, pl.ds(pl.multiple_of(c * width, HD), width)], q.at[pl.ds(c * tok, tok)], load_sem.at[1]
    )
    load_q.start()
    give_q = remote(
        queries.at[:, pl.ds(pl.multiple_of((1 - c) * width, HD), width)],
        q.at[pl.ds(c * tok, tok)], pair_send.at[0], pair_recv.at[0], partner,
    )
    give_q.start()

    def piece(block, a):
        return codes.at[block, pl.ds(pl.multiple_of(parity * half + a * eighth, eighth), eighth)]

    def share(block, a):
        ref = codes.at[block, pl.ds(pl.multiple_of(parity * half + a * quarter, quarter), quarter)]
        dev = across_x + a * (across_y - across_x)
        remote(ref, ref, xy_send.at[0], xy_recv.at[a * nz + block], (dev, s)).start()

    def zm_first(a):
        ref = piece(z, a)
        remote(ref, ref, zm_send.at[0], zm_recv.at[a], down).start()

    def zp_first(a):
        ref = piece(z, a)
        remote(ref, ref, zp_send.at[0], zp_recv.at[a], up).start()

    def zm_step(step, a):
        block = (z + step) % nz
        ref = piece(block, a)
        remote(ref, ref, zm_send.at[0], zm_recv.at[(step - 1) * 4 + a], down).wait_recv()

        @pl.when(step < down_steps)
        def _():
            remote(ref, ref, zm_send.at[0], zm_recv.at[step * 4 + a], down).start()

        @pl.when(a % 2 == 1)
        def _():
            share(block, a // 2)

    def zp_step(step, a):
        block = (z + nz - step) % nz
        ref = piece(block, a)
        remote(ref, ref, zp_send.at[0], zp_recv.at[(step - 1) * 4 + a], up).wait_recv()

        @pl.when(step < up_steps)
        def _():
            remote(ref, ref, zp_send.at[0], zp_recv.at[step * 4 + a], up).start()

        @pl.when(a % 2 == 1)
        def _():
            share(block, a // 2)

    def both_ways(e):
        step, a = e // 4 + 1, e % 4

        @pl.when(step + down_steps_a <= down_steps)
        def _():
            zm_step(step + down_steps_a, a)

        @pl.when(step <= up_steps)
        def _():
            zp_step(step, a)

    load_codes.wait()
    for a in range(4):
        zm_first(a)

    def kv_copy(t, part_index):
        at = t * 4 + part_index
        return remote(kv.at[t, part_index], kv.at[t + 1, part_index], kv_send.at[at], kv_recv.at[at], up)

    def kv_send_from(t, part_index):
        @pl.when((z >= t) & (z < nz - 1))
        def _():
            kv_copy(t, part_index).start()

    for part_index in range(4):
        loads[part_index].wait()
        mine = kv.at[0, part_index, pl.ds((1 - c) * tok, tok)]
        remote(mine, mine, pair_send.at[1 + part_index], pair_recv.at[1 + part_index], partner).wait_recv()
        kv_send_from(0, part_index)
    load_q.wait()
    mine = q.at[pl.ds((1 - c) * tok, tok)]
    remote(mine, mine, pair_send.at[0], pair_recv.at[0], partner).wait_recv()

    factor = math.log2(math.e) / math.sqrt(HD)

    def attend(t, head, group, mode):
        q_rows = q[:, pl.ds(pl.multiple_of(head * HD, HD), HD)]
        scores = lax.dot_general(
            q_rows, kv[t, 2 * group], (((1,), (1,)), ((), ())), preferred_element_type=F32
        )
        if mode != "full":
            i = lax.broadcasted_iota(jnp.int32, (rows, rows), 0)
            j = lax.broadcasted_iota(jnp.int32, (rows, rows), 1)
            scores = jnp.where(j <= i if mode == "own" else j > i, scores, -1e30)
        row_max = jnp.max(scores, axis=1, keepdims=True)
        if mode == "own":
            new_top = jnp.broadcast_to(row_max, (rows, HD))
        else:
            old_top = top[head]
            new_top = jnp.maximum(old_top, row_max)
        top[head] = new_top
        spread = jnp.concatenate([new_top] * (rows // HD), axis=1)
        weights = jnp.exp2((scores - spread) * factor).astype(BF16)
        values = jnp.concatenate([kv[t, 2 * group + 1], jnp.ones((rows, HD), BF16)], axis=1)
        product = jnp.dot(weights, values, preferred_element_type=F32)
        if mode != "own":
            fade = jnp.exp2((old_top - new_top) * factor)
            product = product + acc[head] * jnp.concatenate([fade, fade], axis=1)
        acc[head] = product

    quad = half_heads // 4

    def attend_two(t, index, i, mode):
        head = index * quad + 2 * i
        attend(t, head, index // 2, mode)
        attend(t, head + 1, index // 2, mode)

    def phase_a(t, carry):
        @pl.when(t == hops)
        def _():
            for a in range(4):
                zp_first(a)

        for index in range(4):
            @pl.when(z >= t)
            def _():
                ref = kv.at[t, index]
                remote(ref, ref, kv_send.at[0], kv_recv.at[(t - 1) * 4 + index], up).wait_recv()

            @pl.when(t < hops)
            def _():
                kv_send_from(t, index)

            for i in range(2):
                if index * 2 + i < 7:
                    e = (t - 1) * 7 + index * 2 + i
                    zm_step(e // 4 + 1, e % 4)

                @pl.when(t == 1)
                def _():
                    attend_two(0, index, i, "own")

                @pl.when((t > 1) & (z >= t - 1))
                def _():
                    attend_two(t - 1, index, i, "full")

        return carry

    lax.fori_loop(1, hops + 1, phase_a, 0)

    matrix = had[...]
    stacked = jnp.concatenate([matrix, matrix], axis=0)

    def rotate(head):
        both = acc[head]
        value = both[:, :HD] / both[:, HD:] * signs[pl.ds(c * half_heads + head, 1), :].astype(F32)
        first = value.astype(BF16)
        rest = value - first.astype(F32)
        second = rest.astype(BF16)
        third = (rest - second.astype(F32)).astype(BF16)
        mixed = jnp.dot(jnp.concatenate([first, second], axis=1), stacked, preferred_element_type=F32)
        mixed = mixed + jnp.dot(third, matrix, preferred_element_type=F32)
        column = pl.multiple_of((c * half_heads + head) * HD, HD)
        xr[:, pl.ds(column, HD)] = (mixed * (1.0 / math.sqrt(HD))).astype(BF16)

    def rotate_two(i, carry):
        rotate(2 * i)
        rotate(2 * i + 1)
        return carry

    swap_width = quad * HD

    def swapped(core, index):
        columns = xr.at[:, pl.ds(pl.multiple_of(core * width + index * swap_width, swap_width), swap_width)]
        return remote(columns, columns, xr_send.at[index], xr_recv.at[index], partner)

    def last_quad(index, carry):
        both_ways(2 * index)

        @pl.when(z >= hops)
        def _():
            attend_two(hops, index, 0, "far")
            attend_two(hops, index, 1, "far")

        both_ways(2 * index + 1)

        @pl.when(index > 0)
        def _():
            swapped(c, index - 1).start()

        rotate_two(2 * index, 0)
        rotate_two(2 * index + 1, 0)
        return carry

    lax.fori_loop(0, 4, last_quad, 0)
    both_ways(jnp.int32(8))
    swapped(c, 3).start()
    both_ways(jnp.int32(9))

    pairs = nz // 2
    first_pairs = down_steps_a // 2

    def origins(u):
        late = (u // first_pairs + 1) // 2
        k = u - first_pairs
        one = (1 - late) * 2 * u + late * (down_steps_a + k)
        two = (1 - late) * (2 * u + 1) + late * (nz - 1 - k)
        return (z + one) % nz, (z + two) % nz

    def scale_rows(block):
        column = pl.multiple_of((block * CORES + c) * HD, HD)
        return scales[:, pl.ds(column, HD)].astype(F32)

    def unpack(block, side, weights, rows_of_scales, heads):
        for n in heads:
            packed = codes[block, n * (HD // 8) : (n + 1) * (HD // 8), :] ^ jnp.int32(-2004318072)
            scale = jnp.broadcast_to(rows_of_scales[n : n + 1, :], (HD // 8, HD)).astype(BF16)
            for k in range(8):
                shifted = packed << (28 - 4 * k) if k < 7 else packed
                value = (shifted >> 28).astype(F32).astype(BF16)
                at = n * HD + k * (HD // 8)
                weights[at : at + HD // 8, side * HD : (side + 1) * HD] = value * scale

    def send_out(u):
        for side, block in enumerate(origins(u)):
            columns = pl.ds(pl.multiple_of((block * CORES + c) * HD, HD), HD)
            pltpu.make_async_copy(
                obuf.at[u, side, pl.ds(c * tok, tok)], out.at[:, columns], out_local.at[0]
            ).start()
            remote(
                obuf.at[u, side, pl.ds((1 - c) * tok, tok)], out.at[:, columns], out_send.at[0], out_recv.at[0], partner
            ).start()

    def shared(block):
        for a in range(2):
            ref = codes.at[block, pl.ds(pl.multiple_of((1 - parity) * half + a * quarter, quarter), quarter)]
            dev = across_x if a == 0 else across_y
            remote(ref, ref, xy_send.at[0], xy_recv.at[a * nz + block], (dev, s)).wait_recv()

    def arrived(u):
        one, two = origins(u)

        @pl.when(u > 0)
        def _():
            shared(one)

        shared(two)

    depth = 2 * HD

    def project(u, weights, later):
        both_ways(10 + 2 * u)

        @pl.when(u < pairs - 1)
        def _():
            arrived(u + 1)

        both = origins((u + 1) % pairs)

        def beside(steps, total):
            scale_both = [scale_rows(block) for block in both]
            for n in steps:
                for side in range(2):
                    unpack(both[side], side, later, scale_both[side], (2 * n, 2 * n + 1))
                columns = slice(n * depth, (n + 1) * depth)
                product = jnp.dot(xr[:, columns], weights[columns, :], preferred_element_type=F32)
                total = product if total is None else total + product
            return total

        steps = HEADS // 2
        partial[...] = beside(range(steps // 2), None)
        both_ways(11 + 2 * u)
        total = partial[...] + beside(range(steps // 2, steps), None)
        total = total.astype(BF16)
        obuf[u, 0] = total[:, :HD]
        obuf[u, 1] = total[:, HD:]

        @pl.when(u > 0)
        def _():
            send_out(u - 1)

    def two_pairs(v, carry):
        project(2 * v, weights_even, weights_odd)
        project(2 * v + 1, weights_odd, weights_even)
        return carry

    arrived(jnp.int32(0))
    one, two = origins(jnp.int32(0))
    unpack(one, 0, weights_even, scale_rows(one), range(HEADS))
    unpack(two, 1, weights_even, scale_rows(two), range(HEADS))
    for index in range(4):
        swapped(1 - c, index).wait_recv()
    lax.fori_loop(0, pairs // 2, two_pairs, 0)

    sent = codes.at[pl.ds(0, down_steps), pl.ds(0, half)]
    remote(sent, sent, zm_send.at[0], zm_recv.at[0], down).wait_send()
    sent = codes.at[pl.ds(0, up_steps), pl.ds(0, half)]
    remote(sent, sent, zp_send.at[0], zp_recv.at[0], up).wait_send()
    sent = codes.at[pl.ds(0, nz - 1), pl.ds(0, half)]
    remote(sent, sent, xy_send.at[0], xy_recv.at[0], (across_x, s)).wait_send()

    def kv_left(t, carry):
        @pl.when((z >= t) & (z < nz - 1))
        def _():
            for part_index in range(4):
                kv_copy(t, part_index).wait_send()

        return carry

    lax.fori_loop(0, hops, kv_left, 0)
    give_q.wait_send()
    for index in range(4):
        gives[index].wait_send()
        swapped(c, index).wait_send()
    send_out(pairs - 1)
    moved = obuf.at[:, :, pl.ds(0, tok)]
    pltpu.make_async_copy(moved, moved, out_local.at[0]).wait()
    whole = remote(moved, moved, out_send.at[0], out_recv.at[0], partner)
    whole.wait_send()
    whole.wait_recv()


def plan(nz, hops):
    down_beside = 7 * hops // 4
    up_steps = (nz - 1 - down_beside) // 2 + 1
    return down_beside, up_steps, nz - 1 - up_steps


def on_device(plane_y, queries, keys_values, head_signs, out_codes, out_scales):
    tok = queries.shape[0]
    ns = lax.axis_size("seq")
    nz = ns // CORES
    rows = tok * CORES
    hops = WINDOW // rows
    words, cols = out_codes.shape
    half_heads = HEADS // CORES
    _, up_steps, down_steps = plan(nz, hops)
    kv_rows = keys_values.reshape(tok, 2 * KV * HD)
    had = jnp.asarray(hadamard_columns(), BF16)
    hbm = pl.BlockSpec(memory_space=pltpu.HBM)
    vmem = pl.BlockSpec(memory_space=pltpu.VMEM)
    dma = pltpu.SemaphoreType.DMA
    return pl.pallas_call(
        functools.partial(kernel, plane_y),
        out_shape=jax.ShapeDtypeStruct((tok, ns * cols), BF16),
        in_specs=[hbm, hbm, hbm, vmem, vmem, vmem],
        out_specs=hbm,
        scratch_shapes=[
            pltpu.VMEM((nz, words, cols), jnp.int32),
            pltpu.VMEM((hops + 1, KV, rows, HD), BF16),
            pltpu.VMEM((rows, half_heads * HD), BF16),
            pltpu.VMEM((half_heads, rows, 2 * HD), F32),
            pltpu.VMEM((half_heads, rows, HD), F32),
            pltpu.VMEM((rows, HEADS * HD), BF16),
            pltpu.VMEM((HEADS * HD, 2 * cols), BF16),
            pltpu.VMEM((HEADS * HD, 2 * cols), BF16),
            pltpu.VMEM((rows, 2 * cols), F32),
            pltpu.VMEM((nz // 2, 2, rows, cols), BF16),
            dma((4 * down_steps,)),
            dma((4 * up_steps,)),
            dma((4 * hops,)),
            dma((2 * nz,)),
            dma((1,)),
            dma((1,)),
            dma((4 * hops,)),
            dma((1,)),
            dma((2 + KV,)),
            dma((1 + KV,)),
            dma((1 + KV,)),
            dma((4,)),
            dma((4,)),
            dma((1,)),
            dma((1,)),
            dma((1,)),
        ],
        compiler_params=pltpu.CompilerParams(
            collective_id=0, has_side_effects=True, vmem_limit_bytes=60 * 1024 * 1024
        ),
    )(queries, kv_rows, out_codes, out_scales, head_signs, had)


def solution(mesh):
    groups = mesh.shape["groups"]
    plane_y = 1 << (groups.bit_length() // 2)
    return jax.shard_map(
        functools.partial(on_device, plane_y),
        mesh=mesh,
        in_specs=(
            P(("groups", "seq"), None),
            P(("groups", "seq"), None, None),
            P(),
            P(None, "seq"),
            P(),
        ),
        out_specs=P(("groups", "seq"), None),
        check_vma=False,
    )
```

```python
import functools
import math

import jax
import jax.numpy as jnp
import numpy as np
from jax import lax
from jax.experimental import pallas as pl
from jax.experimental.pallas import tpu as pltpu
from jax.sharding import PartitionSpec as P

HEADS = 32
KV = 4
HD = 128
WINDOW = 2048
CORES = 2
MESH = pl.DeviceIdType.MESH
F32 = jnp.float32
BF16 = jnp.bfloat16


def hadamard_columns():
    d = np.arange(HD)
    e = np.array([8 * i + k for k in range(8) for i in range(HD // 8)])
    common = d[:, None] & e[None, :]
    bits = sum((common >> b) & 1 for b in range(HD.bit_length()))
    return np.where(bits % 2 == 0, 1.0, -1.0).astype(np.float32)


def kernel(
    plane_y,
    queries, kv_in, codes_in, scales, signs, had,
    out,
    codes, kv, q, acc, top, xr, weights_even, weights_odd, partial, obuf,
    zm_recv, zp_recv, kv_recv, xy_recv,
    zm_send, zp_send, kv_send, xy_send,
    load_sem, pair_send, pair_recv, xr_send, xr_recv, out_local, out_send, out_recv,
):
    ns = lax.axis_size("seq")
    nz = ns // CORES
    g = lax.axis_index("groups")
    s = lax.axis_index("seq")
    z = s // CORES
    c = s % CORES
    tok = queries.shape[0]
    rows = tok * CORES
    half_heads = HEADS // CORES
    width = half_heads * HD
    hops = WINDOW // rows
    words = codes_in.shape[0]
    half, quarter, eighth = words // 2, words // 4, words // 8

    gx_, gy_ = g // plane_y, g % plane_y
    across_x = (gx_ + 1 - 2 * (gx_ % 2)) * plane_y + gy_
    across_y = gx_ * plane_y + gy_ + 1 - 2 * (gy_ % 2)
    parity = (gx_ + gy_) % 2
    partner = (g, z * CORES + 1 - c)
    up = (g, (s + CORES) % ns)
    down = (g, (s + ns - CORES) % ns)

    down_steps_a, up_steps, down_steps = plan(nz, hops)

    barrier = pltpu.get_barrier_semaphore()
    for dev in (partner, up, down, (across_x, s), (across_y, s)):
        pl.semaphore_signal(barrier, inc=1, device_id=dev, device_id_type=MESH)
    pl.semaphore_wait(barrier, 5)

    def remote(src, dst, send_sem, recv_sem, dev):
        return pltpu.make_async_remote_copy(
            src_ref=src, dst_ref=dst, send_sem=send_sem, recv_sem=recv_sem, device_id=dev, device_id_type=MESH
        )

    load_codes = pltpu.make_async_copy(codes_in, codes.at[z], load_sem.at[0])
    load_codes.start()
    loads, gives = [], []
    for part_index in range(KV):
        for core, into in ((c, loads), (1 - c, gives)):
            column = (part_index % 2) * KV * HD + (core * (KV // CORES) + part_index // 2) * HD
            source = kv_in.at[:, pl.ds(pl.multiple_of(column, HD), HD)]
            target = kv.at[0, part_index, pl.ds(c * tok, tok)]
            if into is loads:
                copy = pltpu.make_async_copy(source, target, load_sem.at[2 + part_index])
            else:
                copy = remote(source, target, pair_send.at[1 + part_index], pair_recv.at[1 + part_index], partner)
            copy.start()
            into.append(copy)
    load_q = pltpu.make_async_copy(
        queries.at[:, pl.ds(pl.multiple_of(c * width, HD), width)], q.at[pl.ds(c * tok, tok)], load_sem.at[1]
    )
    load_q.start()
    give_q = remote(
        queries.at[:, pl.ds(pl.multiple_of((1 - c) * width, HD), width)],
        q.at[pl.ds(c * tok, tok)], pair_send.at[0], pair_recv.at[0], partner,
    )
    give_q.start()

    def piece(block, a):
        return codes.at[block, pl.ds(pl.multiple_of(parity * half + a * eighth, eighth), eighth)]

    def share(block, a):
        ref = codes.at[block, pl.ds(pl.multiple_of(parity * half + a * quarter, quarter), quarter)]
        dev = across_x + a * (across_y - across_x)
        remote(ref, ref, xy_send.at[0], xy_recv.at[a * nz + block], (dev, s)).start()

    def zm_first(a):
        ref = piece(z, a)
        remote(ref, ref, zm_send.at[0], zm_recv.at[a], down).start()

    def zp_first(a):
        ref = piece(z, a)
        remote(ref, ref, zp_send.at[0], zp_recv.at[a], up).start()

    def zm_step(step, a):
        block = (z + step) % nz
        ref = piece(block, a)
        remote(ref, ref, zm_send.at[0], zm_recv.at[(step - 1) * 4 + a], down).wait_recv()

        @pl.when(step < down_steps)
        def _():
            remote(ref, ref, zm_send.at[0], zm_recv.at[step * 4 + a], down).start()

        @pl.when(a % 2 == 1)
        def _():
            share(block, a // 2)

    def zp_step(step, a):
        block = (z + nz - step) % nz
        ref = piece(block, a)
        remote(ref, ref, zp_send.at[0], zp_recv.at[(step - 1) * 4 + a], up).wait_recv()

        @pl.when(step < up_steps)
        def _():
            remote(ref, ref, zp_send.at[0], zp_recv.at[step * 4 + a], up).start()

        @pl.when(a % 2 == 1)
        def _():
            share(block, a // 2)

    def both_ways(e):
        step, a = e // 4 + 1, e % 4

        @pl.when(step + down_steps_a <= down_steps)
        def _():
            zm_step(step + down_steps_a, a)

        @pl.when(step <= up_steps)
        def _():
            zp_step(step, a)

    load_codes.wait()
    for a in range(4):
        zm_first(a)

    def kv_copy(t, part_index):
        at = t * 4 + part_index
        return remote(kv.at[t, part_index], kv.at[t + 1, part_index], kv_send.at[at], kv_recv.at[at], up)

    def kv_send_from(t, part_index):
        @pl.when((z >= t) & (z < nz - 1))
        def _():
            kv_copy(t, part_index).start()

    for part_index in range(4):
        loads[part_index].wait()
        mine = kv.at[0, part_index, pl.ds((1 - c) * tok, tok)]
        remote(mine, mine, pair_send.at[1 + part_index], pair_recv.at[1 + part_index], partner).wait_recv()
        kv_send_from(0, part_index)
    load_q.wait()
    mine = q.at[pl.ds((1 - c) * tok, tok)]
    remote(mine, mine, pair_send.at[0], pair_recv.at[0], partner).wait_recv()

    factor = math.log2(math.e) / math.sqrt(HD)

    def attend(t, head, group, mode):
        q_rows = q[:, pl.ds(pl.multiple_of(head * HD, HD), HD)]
        scores = lax.dot_general(
            q_rows, kv[t, 2 * group], (((1,), (1,)), ((), ())), preferred_element_type=F32
        )
        if mode != "full":
            i = lax.broadcasted_iota(jnp.int32, (rows, rows), 0)
            j = lax.broadcasted_iota(jnp.int32, (rows, rows), 1)
            scores = jnp.where(j <= i if mode == "own" else j > i, scores, -1e30)
        row_max = jnp.max(scores, axis=1, keepdims=True)
        if mode == "own":
            new_top = jnp.broadcast_to(row_max, (rows, HD))
        else:
            old_top = top[head]
            new_top = jnp.maximum(old_top, row_max)
        top[head] = new_top
        spread = jnp.concatenate([new_top] * (rows // HD), axis=1)
        weights = jnp.exp2((scores - spread) * factor).astype(BF16)
        values = jnp.concatenate([kv[t, 2 * group + 1], jnp.ones((rows, HD), BF16)], axis=1)
        product = jnp.dot(weights, values, preferred_element_type=F32)
        if mode != "own":
            fade = jnp.exp2((old_top - new_top) * factor)
            product = product + acc[head] * jnp.concatenate([fade, fade], axis=1)
        acc[head] = product

    quad = half_heads // 4

    def attend_two(t, index, i, mode):
        head = index * quad + 2 * i
        attend(t, head, index // 2, mode)
        attend(t, head + 1, index // 2, mode)

    def phase_a(t, carry):
        @pl.when(t == hops)
        def _():
            for a in range(4):
                zp_first(a)

        for index in range(4):
            @pl.when(z >= t)
            def _():
                ref = kv.at[t, index]
                remote(ref, ref, kv_send.at[0], kv_recv.at[(t - 1) * 4 + index], up).wait_recv()

            @pl.when(t < hops)
            def _():
                kv_send_from(t, index)

            for i in range(2):
                if index * 2 + i < 7:
                    e = (t - 1) * 7 + index * 2 + i
                    zm_step(e // 4 + 1, e % 4)

                @pl.when(t == 1)
                def _():
                    attend_two(0, index, i, "own")

                @pl.when((t > 1) & (z >= t - 1))
                def _():
                    attend_two(t - 1, index, i, "full")

        return carry

    lax.fori_loop(1, hops + 1, phase_a, 0)

    matrix = had[...]
    stacked = jnp.concatenate([matrix, matrix], axis=0)

    def rotate(head):
        both = acc[head]
        value = both[:, :HD] / both[:, HD:] * signs[pl.ds(c * half_heads + head, 1), :].astype(F32)
        first = value.astype(BF16)
        rest = value - first.astype(F32)
        second = rest.astype(BF16)
        third = (rest - second.astype(F32)).astype(BF16)
        mixed = jnp.dot(jnp.concatenate([first, second], axis=1), stacked, preferred_element_type=F32)
        mixed = mixed + jnp.dot(third, matrix, preferred_element_type=F32)
        column = pl.multiple_of((c * half_heads + head) * HD, HD)
        xr[:, pl.ds(column, HD)] = (mixed * (1.0 / math.sqrt(HD))).astype(BF16)

    def rotate_two(i, carry):
        rotate(2 * i)
        rotate(2 * i + 1)
        return carry

    swap_width = quad * HD

    def swapped(core, index):
        columns = xr.at[:, pl.ds(pl.multiple_of(core * width + index * swap_width, swap_width), swap_width)]
        return remote(columns, columns, xr_send.at[index], xr_recv.at[index], partner)

    def last_quad(index, carry):
        both_ways(2 * index)

        @pl.when(z >= hops)
        def _():
            attend_two(hops, index, 0, "far")
            attend_two(hops, index, 1, "far")

        both_ways(2 * index + 1)

        @pl.when(index > 0)
        def _():
            swapped(c, index - 1).start()

        rotate_two(2 * index, 0)
        rotate_two(2 * index + 1, 0)
        return carry

    lax.fori_loop(0, 4, last_quad, 0)
    swapped(c, 3).start()

    pairs = nz // 2
    first_pairs = down_steps_a // 2

    def origins(u):
        late = (u // first_pairs + 1) // 2
        k = u - first_pairs
        one = (1 - late) * 2 * u + late * (down_steps_a + k)
        two = (1 - late) * (2 * u + 1) + late * (nz - 1 - k)
        return (z + one) % nz, (z + two) % nz

    def scale_rows(block):
        column = pl.multiple_of((block * CORES + c) * HD, HD)
        return scales[:, pl.ds(column, HD)].astype(F32)

    def unpack(block, side, weights, rows_of_scales, heads):
        for n in heads:
            packed = codes[block, n * (HD // 8) : (n + 1) * (HD // 8), :] ^ jnp.int32(-2004318072)
            scale = jnp.broadcast_to(rows_of_scales[n : n + 1, :], (HD // 8, HD)).astype(BF16)
            for k in range(8):
                shifted = packed << (28 - 4 * k) if k < 7 else packed
                value = (shifted >> 28).astype(F32).astype(BF16)
                at = n * HD + k * (HD // 8)
                weights[at : at + HD // 8, side * HD : (side + 1) * HD] = value * scale

    def send_out(u):
        for side, block in enumerate(origins(u)):
            columns = pl.ds(pl.multiple_of((block * CORES + c) * HD, HD), HD)
            pltpu.make_async_copy(
                obuf.at[u, side, pl.ds(c * tok, tok)], out.at[:, columns], out_local.at[0]
            ).start()
            remote(
                obuf.at[u, side, pl.ds((1 - c) * tok, tok)], out.at[:, columns], out_send.at[0], out_recv.at[0], partner
            ).start()

    def shared(block):
        for a in range(2):
            ref = codes.at[block, pl.ds(pl.multiple_of((1 - parity) * half + a * quarter, quarter), quarter)]
            dev = across_x if a == 0 else across_y
            remote(ref, ref, xy_send.at[0], xy_recv.at[a * nz + block], (dev, s)).wait_recv()

    def arrived(u):
        one, two = origins(u)

        @pl.when(u > 0)
        def _():
            shared(one)

        shared(two)

    depth = 2 * HD

    def project(u, weights, later):
        both_ways(8 + 2 * u)

        @pl.when(u < pairs - 1)
        def _():
            arrived(u + 1)

        both = origins((u + 1) % pairs)

        def beside(steps, total):
            scale_both = [scale_rows(block) for block in both]
            for n in steps:
                for side in range(2):
                    unpack(both[side], side, later, scale_both[side], (2 * n, 2 * n + 1))
                columns = slice(n * depth, (n + 1) * depth)
                product = jnp.dot(xr[:, columns], weights[columns, :], preferred_element_type=F32)
                total = product if total is None else total + product
            return total

        steps = HEADS // 2
        partial[...] = beside(range(steps // 2), None)
        both_ways(9 + 2 * u)
        total = partial[...] + beside(range(steps // 2, steps), None)
        total = total.astype(BF16)
        obuf[u, 0] = total[:, :HD]
        obuf[u, 1] = total[:, HD:]

        @pl.when(u > 0)
        def _():
            send_out(u - 1)

    def two_pairs(v, carry):
        project(2 * v, weights_even, weights_odd)
        project(2 * v + 1, weights_odd, weights_even)
        return carry

    arrived(jnp.int32(0))
    one, two = origins(jnp.int32(0))
    unpack(one, 0, weights_even, scale_rows(one), range(HEADS))
    unpack(two, 1, weights_even, scale_rows(two), range(HEADS))
    for index in range(4):
        swapped(1 - c, index).wait_recv()
    lax.fori_loop(0, pairs // 2, two_pairs, 0)

    sent = codes.at[pl.ds(0, down_steps), pl.ds(0, half)]
    remote(sent, sent, zm_send.at[0], zm_recv.at[0], down).wait_send()
    sent = codes.at[pl.ds(0, up_steps), pl.ds(0, half)]
    remote(sent, sent, zp_send.at[0], zp_recv.at[0], up).wait_send()
    sent = codes.at[pl.ds(0, nz - 1), pl.ds(0, half)]
    remote(sent, sent, xy_send.at[0], xy_recv.at[0], (across_x, s)).wait_send()

    def kv_left(t, carry):
        @pl.when((z >= t) & (z < nz - 1))
        def _():
            for part_index in range(4):
                kv_copy(t, part_index).wait_send()

        return carry

    lax.fori_loop(0, hops, kv_left, 0)
    give_q.wait_send()
    for index in range(4):
        gives[index].wait_send()
        swapped(c, index).wait_send()
    send_out(pairs - 1)
    moved = obuf.at[:, :, pl.ds(0, tok)]
    pltpu.make_async_copy(moved, moved, out_local.at[0]).wait()
    whole = remote(moved, moved, out_send.at[0], out_recv.at[0], partner)
    whole.wait_send()
    whole.wait_recv()


def plan(nz, hops):
    down_beside = 7 * hops // 4
    up_steps = (nz - 1 - down_beside) // 2 + 1
    return down_beside, up_steps, nz - 1 - up_steps


def on_device(plane_y, queries, keys_values, head_signs, out_codes, out_scales):
    tok = queries.shape[0]
    ns = lax.axis_size("seq")
    nz = ns // CORES
    rows = tok * CORES
    hops = WINDOW // rows
    words, cols = out_codes.shape
    half_heads = HEADS // CORES
    _, up_steps, down_steps = plan(nz, hops)
    kv_rows = keys_values.reshape(tok, 2 * KV * HD)
    had = jnp.asarray(hadamard_columns(), BF16)
    hbm = pl.BlockSpec(memory_space=pltpu.HBM)
    vmem = pl.BlockSpec(memory_space=pltpu.VMEM)
    dma = pltpu.SemaphoreType.DMA
    return pl.pallas_call(
        functools.partial(kernel, plane_y),
        out_shape=jax.ShapeDtypeStruct((tok, ns * cols), BF16),
        in_specs=[hbm, hbm, hbm, vmem, vmem, vmem],
        out_specs=hbm,
        scratch_shapes=[
            pltpu.VMEM((nz, words, cols), jnp.int32),
            pltpu.VMEM((hops + 1, KV, rows, HD), BF16),
            pltpu.VMEM((rows, half_heads * HD), BF16),
            pltpu.VMEM((half_heads, rows, 2 * HD), F32),
            pltpu.VMEM((half_heads, rows, HD), F32),
            pltpu.VMEM((rows, HEADS * HD), BF16),
            pltpu.VMEM((HEADS * HD, 2 * cols), BF16),
            pltpu.VMEM((HEADS * HD, 2 * cols), BF16),
            pltpu.VMEM((rows, 2 * cols), F32),
            pltpu.VMEM((nz // 2, 2, rows, cols), BF16),
            dma((4 * down_steps,)),
            dma((4 * up_steps,)),
            dma((4 * hops,)),
            dma((2 * nz,)),
            dma((1,)),
            dma((1,)),
            dma((4 * hops,)),
            dma((1,)),
            dma((2 + KV,)),
            dma((1 + KV,)),
            dma((1 + KV,)),
            dma((4,)),
            dma((4,)),
            dma((1,)),
            dma((1,)),
            dma((1,)),
        ],
        compiler_params=pltpu.CompilerParams(
            collective_id=0, has_side_effects=True, vmem_limit_bytes=60 * 1024 * 1024
        ),
    )(queries, kv_rows, out_codes, out_scales, head_signs, had)


def solution(mesh):
    groups = mesh.shape["groups"]
    plane_y = 1 << (groups.bit_length() // 2)
    return jax.shard_map(
        functools.partial(on_device, plane_y),
        mesh=mesh,
        in_specs=(
            P(("groups", "seq"), None),
            P(("groups", "seq"), None, None),
            P(),
            P(None, "seq"),
            P(),
        ),
        out_specs=P(("groups", "seq"), None),
        check_vma=False,
    )
```
